1024 devices in a mesh: grp: 16 (over y_hi, x, core), dp: 64 (over z, y_lo).
Axes of the slice: x: 4, y: 4 (y_hi: 2, y_lo: 2; y = y_hi * 2 + y_lo), z: 32, core: 2. Of those that a mesh axis runs over, the one named last changes fastest.
Arguments:
- query: bfloat16 [64, 2048, 2560], P('dp', 'grp'), may hold values from -30 to 30
- resp_kv: bfloat16 [64, 2048, 1024], P('dp', 'grp'), may hold values from -6 to 6
- prefix_kv: bfloat16 [64, 256, 1024], P('dp', 'grp'), may hold values from -30 to 30
- query_bias: float32 [2560], replicated, may hold values from -3 to 3
- kv_bias: float32 [1024], replicated, may hold values from -3 to 3
- out_grad: bfloat16 [64, 2048, 2560], P('dp', 'grp'), may hold values from -6 to 6
- lengths: int32 [64, 16], P('dp', 'grp'), may hold values from 32 to 128
Outputs:
- attended: bfloat16 [64, 2048, 2560], P('dp', 'grp')
- query_grad: bfloat16 [64, 2048, 2560], P('dp', 'grp')
- resp_kv_grad: bfloat16 [64, 2048, 1024], P('dp', 'grp')
- prefix_kv_grad: bfloat16 [64, 256, 1024], P('dp', 'grp')
- query_bias_grad: float32 [2560], replicated
- kv_bias_grad: float32 [1024], replicated
The draws below stay inside these ranges and needn't reach their ends.
All inputs are finite; a program needn't handle non-finite values.
Results may differ from the reference program's by a relative error of at most 0.013.
The reference program's roundings to bfloat16 on the way count: a program that leaves them out, or rounds other values in their place, can miss the bound.
Values may be sent and summed in bfloat16 or wider, within the bound.
No kernel may reach another device: no remote copies, remote signals or barrier semaphores. Data moves between devices by JAX's collectives and lax.ppermute only.
A program may use at most 32 MiB of HBM per device.

```python
import jax
import jax.numpy as jnp
from jax import lax

QH = 20
KVH = 4
HD = 128
RESP = 128
PRE = 256
RESP_ALL = 2048
PROMPTS = 64
N_GRP = 16


def make_pair(key):
    base = jax.random.fold_in(key, 7)
    first, second = jax.random.split(base, 2)
    queries = jax.random.normal(first, (PROMPTS, RESP_ALL, QH * HD), jnp.float32)
    prefix = jax.random.normal(second, (PROMPTS, PRE, 2 * KVH * HD), jnp.float32)
    return (jnp.clip(queries, -6.0, 6.0), jnp.clip(prefix, -6.0, 6.0))


def draw_query(key, part):
    return make_pair(key)[0].astype(jnp.bfloat16)


def draw_prefix_kv(key, part):
    return make_pair(key)[1].astype(jnp.bfloat16)


def plant(values, rng, low, high):
    place = [jax.random.randint(jax.random.fold_in(rng, axis), (), 0, length) for axis, length in enumerate(values.shape)]
    main_axis = values.shape.index(max(values.shape))
    beside = place[:main_axis] + [(place[main_axis] + 1) % values.shape[main_axis]] + place[main_axis + 1:]
    return values.at[tuple(place)].set(low).at[tuple(beside)].set(high)


def shard_levels(stream_key, extent, cuts, low, top_value):
    gain, own = 1.0, jax.random.fold_in(stream_key, 6)
    for dim, parts in cuts:
        heights = jnp.exp(jax.random.uniform(jax.random.fold_in(own, dim), (parts,), jnp.float32, low / len(cuts), top_value / len(cuts)))
        gain = gain * jnp.repeat(heights, extent[dim] // parts).reshape([-1 if axis == dim else 1 for axis in range(len(extent))])
    return gain


def normal_values(own_key, shape, deviation, limit, cuts=(), kind=jnp.bfloat16):
    entries = jax.random.normal(own_key, shape, jnp.float32) * deviation
    if len(cuts) > 0:
        entries = shard_levels(own_key, shape, cuts, -0.22, 0.18) * entries
    return jnp.clip(entries, min=-limit, max=limit).astype(kind)


def setup_inputs(seed: int = 0) -> dict:
    splits = jax.random.split(jax.random.key(seed), 8)
    return {
        "query": draw_query(jax.random.fold_in(splits[7], 71), 0),
        "resp_kv": normal_values(splits[1], (PROMPTS, RESP_ALL, 2 * KVH * HD), 1.0, 6.0, ((0, 64), (1, 16))),
        "prefix_kv": draw_prefix_kv(jax.random.fold_in(splits[7], 71), 0),
        "query_bias": normal_values(splits[3], (QH * HD,), 0.5, 3.0, (), jnp.float32),
        "kv_bias": normal_values(splits[4], (2 * KVH * HD,), 0.5, 3.0, (), jnp.float32),
        "out_grad": normal_values(splits[5], (PROMPTS, RESP_ALL, QH * HD), 1.0, 6.0, ((0, 64), (1, 16))),
        "lengths": plant(jax.random.randint(splits[6], (PROMPTS, N_GRP), RESP // 4, RESP + 1), jax.random.fold_in(splits[6], 1), RESP // 4, RESP).astype(jnp.int32),
    }


NEG_BIG = -1e30


def attend_group(queries, cotangent, key_blocks, value_blocks, allows):
    factor = queries.shape[-1] ** -0.5
    query_f = queries.astype(jnp.float32)
    grad_f = cotangent.astype(jnp.float32)
    scores = []
    for keys, allow in zip(key_blocks, allows):
        raw = jnp.einsum("thd,sd->hts", query_f, keys.astype(jnp.float32)) * factor
        scores.append(jnp.where(allow[None], raw, NEG_BIG))
    highest = jnp.max(scores[0], -1, keepdims=True)
    for item in scores[1:]:
        highest = jnp.maximum(highest, jnp.max(item, -1, keepdims=True))
    powers = [jnp.exp(item - highest) for item in scores]
    totals = sum(jnp.sum(item, -1, keepdims=True) for item in powers)
    chances = [item / totals for item in powers]
    rounded = [item.astype(jnp.bfloat16) for item in chances]
    output = sum(jnp.einsum("hts,sd->thd", wts.astype(jnp.float32), vals.astype(jnp.float32)) for wts, vals in zip(rounded, value_blocks))
    slopes = [jnp.einsum("thd,sd->hts", grad_f, vals.astype(jnp.float32)) for vals in value_blocks]
    row_dot = sum(jnp.sum(prob * slope, -1, keepdims=True) for prob, slope in zip(chances, slopes))
    shifted = [(prob * (slope - row_dot)).astype(jnp.bfloat16) for prob, slope in zip(chances, slopes)]
    query_grad = sum(jnp.einsum("hts,sd->thd", dsb.astype(jnp.float32), keys.astype(jnp.float32)) for dsb, keys in zip(shifted, key_blocks)) * factor
    key_grads = [jnp.einsum("hts,thd->sd", dsb.astype(jnp.float32), query_f) * factor for dsb in shifted]
    value_grads = [jnp.einsum("hts,thd->sd", wts.astype(jnp.float32), grad_f) for wts in rounded]
    return output, query_grad, key_grads, value_grads


def one_response(query, resp_kv, prefix, cotangent, length, query_bias, kv_bias):
    slots = query.shape[0]
    pre_rows = prefix.shape[0]
    group = QH // KVH
    width = KVH * HD
    biased_query = (query.astype(jnp.float32) + query_bias).astype(jnp.bfloat16)
    own_kv = (resp_kv.astype(jnp.float32) + kv_bias).astype(jnp.bfloat16)
    position = jnp.arange(slots, dtype=jnp.int32)
    live = position < length
    grad_live = jnp.where(live[:, None], cotangent, jnp.zeros_like(cotangent))
    allow_own = position[None, :] <= position[:, None]
    allow_pre = jnp.ones((slots, pre_rows), dtype=bool)
    queries = biased_query.reshape(slots, KVH, group, HD).transpose(1, 0, 2, 3)
    grads = grad_live.reshape(slots, KVH, group, HD).transpose(1, 0, 2, 3)
    pre_keys = prefix[:, :width].reshape(pre_rows, KVH, HD).transpose(1, 0, 2)
    pre_vals = prefix[:, width:].reshape(pre_rows, KVH, HD).transpose(1, 0, 2)
    own_keys = own_kv[:, :width].reshape(slots, KVH, HD).transpose(1, 0, 2)
    own_vals = own_kv[:, width:].reshape(slots, KVH, HD).transpose(1, 0, 2)

    def per_group(pieces):
        qpart, gpart, pkey, pval, okey, oval = pieces
        output, qgrad, kgrads, vgrads = attend_group(qpart, gpart, [pkey, okey], [pval, oval], [allow_pre, allow_own])
        return output, qgrad, kgrads[0], vgrads[0], kgrads[1], vgrads[1]

    output, qgrad, pk_grad, pv_grad, ok_grad, ov_grad = lax.map(per_group, (queries, grads, pre_keys, pre_vals, own_keys, own_vals))
    output = output.transpose(1, 0, 2, 3).reshape(slots, QH * HD)
    attended = jnp.where(live[:, None], output, 0.0).astype(jnp.bfloat16)
    qgrad = qgrad.transpose(1, 0, 2, 3).reshape(slots, QH * HD)
    own_grad = jnp.concatenate([ok_grad.transpose(1, 0, 2).reshape(slots, width), ov_grad.transpose(1, 0, 2).reshape(slots, width)], -1)
    pre_grad = jnp.concatenate([pk_grad.transpose(1, 0, 2).reshape(pre_rows, width), pv_grad.transpose(1, 0, 2).reshape(pre_rows, width)], -1)
    return attended, qgrad, own_grad, pre_grad


def reference(query, resp_kv, prefix_kv, query_bias, kv_bias, out_grad, lengths):
    def prompt(pieces):
        qpart, rpart, ppart, gpart, lpart = pieces
        prefix = (ppart.astype(jnp.float32) + kv_bias).astype(jnp.bfloat16)
        qsplit = qpart.reshape(N_GRP, RESP, QH * HD)
        rsplit = rpart.reshape(N_GRP, RESP, 2 * KVH * HD)
        gsplit = gpart.reshape(N_GRP, RESP, QH * HD)

        def single(qone, rone, gone, lone):
            return one_response(qone, rone, prefix, gone, lone, query_bias, kv_bias)

        attended, qgrad, own_grad, pre_grad = jax.vmap(single)(qsplit, rsplit, gsplit, lpart)
        held = lax.optimization_barrier(pre_grad.astype(jnp.bfloat16))
        pre_sum = jnp.sum(held.astype(jnp.float32), 0).astype(jnp.bfloat16)
        qsum = jnp.sum(qgrad, (0, 1))
        kvsum = jnp.sum(own_grad, (0, 1)) + jnp.sum(pre_grad, (0, 1))
        return (attended.reshape(RESP_ALL, QH * HD), qgrad.astype(jnp.bfloat16).reshape(RESP_ALL, QH * HD),
                own_grad.astype(jnp.bfloat16).reshape(RESP_ALL, 2 * KVH * HD), pre_sum, qsum, kvsum)

    result = lax.map(prompt, (query, resp_kv, prefix_kv, out_grad, lengths))
    return result[0], result[1], result[2], result[3], jnp.sum(result[4], 0), jnp.sum(result[5], 0)
```

```python
import jax
import jax.numpy as jnp
from jax import lax
from jax.experimental import pallas as pl
from jax.experimental.pallas import tpu as pltpu
from jax.sharding import Mesh
from jax.sharding import PartitionSpec as P

QH = 20
KVH = 4
HD = 128
RESP = 128
PRE = 256
KEYS = PRE + RESP
GROUP = QH // KVH
WIDTH = KVH * HD
GW = GROUP * HD
PEERS = 16
ROWS = PRE // PEERS
CHUNK = 2 * KVH * ROWS
FACTOR = HD ** (-0.5)
SCALE = FACTOR * 1.4426950408889634
GRP = ("grp_0", "grp_1", "grp_2")
DP = ("dp_0", "dp_1")
PLANE = ("grp_0", "grp_1", "grp_2", "dp_1")
COLUMN = "dp_0"
NEG_BIG = -1e30
VMEM_LIMIT = 24 * 1024 * 1024
BF16 = jnp.bfloat16
F32 = jnp.float32


def dot(a, b, contract):
    return lax.dot_general(a, b, (contract, ((), ())), preferred_element_type=F32)


def in_three(x):
    high = x.astype(BF16).astype(F32)
    rest = x - high
    middle = rest.astype(BF16).astype(F32)
    return high, middle, rest - middle


def stacked(ref):
    return jnp.concatenate([ref[:, h * HD:(h + 1) * HD] for h in range(GROUP)], 0)


def row_sum(weights, rows):
    parts = jnp.concatenate([*in_three(weights), jnp.zeros((5, weights.shape[1]), F32)], 0)
    return jnp.sum(dot(parts.astype(BF16), rows, ((1,), (0,))), 0, keepdims=True)


def biased(values, bias_ref, index):
    return (values.astype(F32) + bias_ref[pl.ds(index, 1), :]).astype(BF16)


def raw_pair(both, q, g):
    zero = jnp.zeros((RESP, HD), BF16)
    pair = jnp.concatenate([jnp.concatenate([q, zero], 1), jnp.concatenate([zero, g], 1)], 0)
    return dot(both, pair, ((1,), (1,)))


def own_kernel(len_ref, query_ref, grad_ref, k_ref, v_ref, qb_ref, kb_ref,
               q_ref, g_ref, own_ref, e_ref, dp_ref, stat_ref):
    j = pl.program_id(0)
    live = lax.broadcasted_iota(jnp.int32, (RESP, HD), 0) < len_ref[0, 0]
    for h in range(GROUP):
        cols = slice(h * HD, (h + 1) * HD)
        q_ref[:, cols] = biased(query_ref[:, cols], qb_ref, j * GROUP + h)
        g_ref[:, cols] = jnp.where(live, grad_ref[:, cols].astype(F32), 0.0).astype(BF16)
    keys = biased(k_ref[...], kb_ref, j)
    vals = biased(v_ref[...], kb_ref, KVH + j)
    col = pl.multiple_of(j * HD, HD)
    own_ref[:, pl.ds(col, HD)] = keys
    own_ref[:, pl.ds(col + WIDTH, HD)] = vals
    both = jnp.concatenate([keys, vals], 1)
    allow = lax.broadcasted_iota(jnp.int32, (RESP, RESP), 0) <= lax.broadcasted_iota(jnp.int32, (RESP, RESP), 1)
    for h in range(GROUP):
        cols = slice(h * HD, (h + 1) * HD)
        raw = raw_pair(both, q_ref[:, cols], g_ref[:, cols])
        s = jnp.where(allow, raw[:, :RESP], NEG_BIG)
        dp = raw[:, RESP:]
        top = jnp.max(s, 0, keepdims=True)
        e = jnp.exp2((s - top) * SCALE)
        e_ref[:, cols] = e
        dp_ref[:, cols] = dp
        stat_ref[0, 0:1, cols] = top
        stat_ref[0, 1:2, cols] = jnp.sum(e, 0, keepdims=True)
        stat_ref[0, 2:3, cols] = jnp.sum(e * dp, 0, keepdims=True)
        stat_ref[0, 3:8, cols] = jnp.zeros((5, HD), F32)


STEP = 64


def fold(x, how):
    return how(x.reshape(-1, 8, HD), 0)


def score_kernel(q_ref, g_ref, pk_ref, pv_ref, kb_ref, own_ref, e_ref, dp_ref, stat_ref, bias_ref, raw_ref, ds_ref):
    j = pl.program_id(0)
    keys = biased(pk_ref[...], kb_ref, j)
    both = jnp.concatenate([keys, biased(pv_ref[...], kb_ref, KVH + j)], 1)
    for h in range(GROUP):
        cols = slice(h * HD, (h + 1) * HD)
        raw_ref[h] = raw_pair(both, q_ref[:, cols], g_ref[:, cols])
    shift_sums = []
    prob_sums = []
    for h in range(GROUP):
        cols = slice(h * HD, (h + 1) * HD)
        own_top = stat_ref[0, 0:1, cols]
        high = jnp.full((8, HD), NEG_BIG, F32)
        for at in range(0, PRE, STEP):
            high = jnp.maximum(high, fold(raw_ref[h, at:at + STEP, :RESP], jnp.max))
        top = jnp.maximum(own_top, jnp.max(high, 0, keepdims=True))
        total = jnp.zeros((8, HD), F32)
        meet = jnp.zeros((8, HD), F32)
        for at in range(0, PRE, STEP):
            e = jnp.exp2((raw_ref[h, at:at + STEP, :RESP] - top) * SCALE)
            raw_ref[h, at:at + STEP, :RESP] = e
            total = total + fold(e, jnp.sum)
            meet = meet + fold(e * raw_ref[h, at:at + STEP, RESP:], jnp.sum)
        fade = jnp.exp2((own_top - top) * SCALE)
        inverse = 1.0 / (stat_ref[0, 1:2, cols] * fade + jnp.sum(total, 0, keepdims=True))
        row = (stat_ref[0, 2:3, cols] * fade + jnp.sum(meet, 0, keepdims=True)) * inverse
        own_inverse = fade * inverse
        prob_sum = jnp.zeros((8, HD), F32)
        shift_sum = jnp.zeros((8, HD), F32)
        for at in range(0, KEYS, STEP):
            if at < PRE:
                p = raw_ref[h, at:at + STEP, :RESP] * inverse
                dp = raw_ref[h, at:at + STEP, RESP:]
            else:
                p = e_ref[at - PRE:at - PRE + STEP, cols] * own_inverse
                dp = dp_ref[at - PRE:at - PRE + STEP, cols]
            pb = p.astype(BF16)
            dsb = (p * (dp - row)).astype(BF16)
            ds_ref[at:at + STEP, cols] = dsb
            prob_sum = prob_sum + fold(pb.astype(F32), jnp.sum)
            shift_sum = shift_sum + fold(dsb.astype(F32), jnp.sum)
        prob_sums.append(jnp.sum(prob_sum, 0, keepdims=True))
        shift_sums.append(jnp.sum(shift_sum, 0, keepdims=True))

    def put(index, value):
        for copy in range(2):
            bias_ref[pl.ds(2 * (index // 2) + copy, 1), pl.ds(index % 2, 1), :] = value.reshape(1, 1, HD)

    dq = dot(ds_ref[...], jnp.concatenate([keys, own_ref[...]], 0), ((0,), (0,))) * FACTOR
    for h in range(GROUP):
        put(j * GROUP + h, jnp.sum(dq[h * RESP:(h + 1) * RESP], 0, keepdims=True))
    put(QH + j, row_sum(jnp.concatenate(shift_sums, 1), stacked(q_ref)) * FACTOR)
    put(QH + KVH + j, row_sum(jnp.concatenate(prob_sums, 1), stacked(g_ref)))
    put(QH + 2 * KVH + j, jnp.zeros((1, HD), F32))


def grad_kernel(len_ref, q_ref, g_ref, pk_ref, pv_ref, kb_ref, ok_ref, ov_ref,
                att_ref, dq_ref, own_ref, pre_ref, pt_ref, ds_ref):
    j = pl.program_id(0)
    keys = jnp.concatenate([biased(pk_ref[...], kb_ref, j), ok_ref[...]], 0)
    vals = jnp.concatenate([biased(pv_ref[...], kb_ref, KVH + j), ov_ref[...]], 0)
    both = jnp.concatenate([keys, vals], 1)
    allow = lax.broadcasted_iota(jnp.int32, (RESP, RESP), 0) <= lax.broadcasted_iota(jnp.int32, (RESP, RESP), 1)
    for h in range(GROUP):
        cols = slice(h * HD, (h + 1) * HD)
        raw = raw_pair(both, q_ref[:, cols], g_ref[:, cols])
        s = raw[:, :RESP]
        dp = raw[:, RESP:]
        s = jnp.concatenate([s[:PRE], jnp.where(allow, s[PRE:], NEG_BIG)], 0)
        e = jnp.exp2((s - jnp.max(s, 0, keepdims=True)) * SCALE)
        p = e * (1.0 / jnp.sum(e, 0, keepdims=True))
        row = jnp.sum(p * dp, 0, keepdims=True)
        pt_ref[:, cols] = p.astype(BF16)
        ds_ref[:, cols] = (p * (dp - row)).astype(BF16)
    pt = pt_ref[...]
    ds = ds_ref[...]
    dk = dot(ds, stacked(q_ref), ((1,), (0,))) * FACTOR
    dv = dot(pt, stacked(g_ref), ((1,), (0,)))
    col = pl.multiple_of(j * HD, HD)
    own_ref[:, pl.ds(col, HD)] = dk[PRE:].astype(BF16)
    own_ref[:, pl.ds(col + WIDTH, HD)] = dv[PRE:].astype(BF16)
    at = pl.multiple_of(j * ROWS, ROWS)
    pre_ref[:, pl.ds(at, ROWS), :] = dk[:PRE].astype(BF16).reshape(PEERS, ROWS, HD)
    pre_ref[:, pl.ds(at + KVH * ROWS, ROWS), :] = dv[:PRE].astype(BF16).reshape(PEERS, ROWS, HD)
    dq = dot(ds, keys, ((0,), (0,))) * FACTOR
    out = dot(pt, vals, ((0,), (0,)))
    live = lax.broadcasted_iota(jnp.int32, (RESP, HD), 0) < len_ref[0, 0]
    for h in range(GROUP):
        cols = slice(h * HD, (h + 1) * HD)
        rows = slice(h * RESP, (h + 1) * RESP)
        att_ref[:, cols] = jnp.where(live, out[rows], 0.0).astype(BF16)
        dq_ref[:, cols] = dq[rows].astype(BF16)


def enclose_kernel(buffer_ref, parts_ref, out_ref):
    del buffer_ref
    total = jnp.sum(parts_ref[...], 0)
    rows = jnp.concatenate([*in_three(total), jnp.zeros((2, HD), F32)], 0).astype(BF16)
    out_ref[...] = jnp.broadcast_to(rows[None], (PEERS, 8, HD))


def finish_kernel(arrived_ref, pre_ref, q_ref, kv_ref):
    for m in range(2 * KVH):
        piece = arrived_ref[:, m * ROWS:(m + 1) * ROWS, :].astype(F32)
        pre_ref[:, m * HD:(m + 1) * HD] = jnp.sum(piece, 0).astype(BF16)
    for i in range((QH + 2 * KVH) // 2):
        tail = arrived_ref[i, CHUNK:, :].astype(F32)
        pair = tail[0:2] + tail[2:4] + tail[4:6]
        if 2 * i < QH:
            q_ref[2 * i:2 * i + 2, :] = pair
        else:
            kv_ref[2 * i - QH:2 * i - QH + 2, :] = pair


def first(j):
    return 0, j


def second(j):
    return 0, KVH + j


def whole(j):
    return 0, 0


def params():
    return pltpu.CompilerParams(dimension_semantics=("arbitrary",), vmem_limit_bytes=VMEM_LIMIT)


def cost(matmuls):
    return pl.CostEstimate(
        flops=matmuls * 2 * QH * RESP * KEYS * HD, bytes_accessed=4_000_000, transcendentals=QH * RESP * KEYS
    )


def own(length, query, out_grad, resp_kv, query_bias, kv_bias):
    wide = pl.BlockSpec((RESP, GW), first)
    return pl.pallas_call(
        own_kernel,
        grid=(KVH,),
        in_specs=[
            pl.BlockSpec(memory_space=pltpu.SMEM),
            wide,
            wide,
            pl.BlockSpec((RESP, HD), first),
            pl.BlockSpec((RESP, HD), second),
            pl.BlockSpec((QH, HD), whole),
            pl.BlockSpec((2 * KVH, HD), whole),
        ],
        out_specs=[
            wide,
            wide,
            pl.BlockSpec((RESP, 2 * WIDTH), lambda j: (0, 0)),
            wide,
            wide,
            pl.BlockSpec((1, 8, GW), lambda j: (j, 0, 0)),
        ],
        out_shape=[
            jax.ShapeDtypeStruct((RESP, QH * HD), BF16),
            jax.ShapeDtypeStruct((RESP, QH * HD), BF16),
            jax.ShapeDtypeStruct((RESP, 2 * WIDTH), BF16),
            pltpu.HBM((RESP, QH * HD), F32),
            pltpu.HBM((RESP, QH * HD), F32),
            jax.ShapeDtypeStruct((KVH, 8, GW), F32),
        ],
        compiler_params=params(),
        cost_estimate=cost(1),
        name="own",
    )(length, query, out_grad, resp_kv, resp_kv, query_bias, kv_bias)


def score(q, g, prefix, kv_bias, own_kv, e, dp, stat):
    wide = pl.BlockSpec((RESP, GW), first)
    return pl.pallas_call(
        score_kernel,
        grid=(KVH,),
        in_specs=[
            wide,
            wide,
            pl.BlockSpec((PRE, HD), first),
            pl.BlockSpec((PRE, HD), second),
            pl.BlockSpec((2 * KVH, HD), whole),
            pl.BlockSpec((RESP, HD), first),
            wide,
            wide,
            pl.BlockSpec((1, 8, GW), lambda j: (j, 0, 0)),
        ],
        out_specs=pl.BlockSpec((32, 2, HD), lambda j: (0, 0, 0)),
        out_shape=jax.ShapeDtypeStruct((32, 2, HD), F32),
        scratch_shapes=[pltpu.VMEM((GROUP, PRE, 2 * RESP), F32), pltpu.VMEM((KEYS, GW), BF16)],
        compiler_params=params(),
        cost_estimate=cost(3),
        name="score",
    )(q, g, prefix, prefix, kv_bias, own_kv, e, dp, stat)


def grads(length, q, g, prefix, kv_bias, own_kv):
    wide = pl.BlockSpec((RESP, GW), first)
    return pl.pallas_call(
        grad_kernel,
        grid=(KVH,),
        in_specs=[
            pl.BlockSpec(memory_space=pltpu.SMEM),
            wide,
            wide,
            pl.BlockSpec((PRE, HD), first),
            pl.BlockSpec((PRE, HD), second),
            pl.BlockSpec((2 * KVH, HD), whole),
            pl.BlockSpec((RESP, HD), first),
            pl.BlockSpec((RESP, HD), second),
        ],
        out_specs=[
            wide,
            wide,
            pl.BlockSpec((RESP, 2 * WIDTH), whole),
            pl.BlockSpec((PEERS, CHUNK + 8, HD), lambda j: (0, 0, 0)),
        ],
        out_shape=[
            jax.ShapeDtypeStruct((RESP, QH * HD), BF16),
            jax.ShapeDtypeStruct((RESP, QH * HD), BF16),
            jax.ShapeDtypeStruct((RESP, 2 * WIDTH), BF16),
            jax.ShapeDtypeStruct((PEERS, CHUNK + 8, HD), BF16),
        ],
        scratch_shapes=[pltpu.VMEM((KEYS, GW), BF16), pltpu.VMEM((KEYS, GW), BF16)],
        compiler_params=params(),
        cost_estimate=cost(6),
        name="grads",
    )(length, q, g, prefix, prefix, kv_bias, own_kv, own_kv)


def enclose(pre, parts):
    return pl.pallas_call(
        enclose_kernel,
        grid=(1,),
        in_specs=[pl.BlockSpec(memory_space=pl.ANY), pl.BlockSpec((32, 2, HD), lambda i: (0, 0, 0))],
        out_specs=pl.BlockSpec((PEERS, 8, HD), lambda i: (0, CHUNK // 8, 0)),
        out_shape=jax.ShapeDtypeStruct(pre.shape, BF16),
        input_output_aliases={0: 0},
        compiler_params=params(),
        name="enclose",
    )(pre, parts)


def finish(arrived):
    return pl.pallas_call(
        finish_kernel,
        out_shape=[
            jax.ShapeDtypeStruct((ROWS, 2 * WIDTH), BF16),
            jax.ShapeDtypeStruct((QH, HD), F32),
            jax.ShapeDtypeStruct((2 * KVH, HD), F32),
        ],
        compiler_params=pltpu.CompilerParams(vmem_limit_bytes=VMEM_LIMIT),
        name="finish",
    )(arrived)


def in_hbm(x):
    return pltpu.with_memory_space_constraint(x, pltpu.HBM)


def exchange(pieces, axes):
    return lax.all_to_all(pieces, axes, 0, 0, tiled=True)


def local(query, resp_kv, prefix_kv, query_bias, kv_bias, out_grad, lengths):
    query_bias = query_bias.reshape(QH, HD)
    kv_bias = kv_bias.reshape(2 * KVH, HD)
    prefix = exchange(jnp.broadcast_to(prefix_kv[0], (PEERS, ROWS, 2 * WIDTH)), GRP).reshape(PRE, 2 * WIDTH)
    q, g, own_kv, e, dp, stat = own(lengths, in_hbm(query[0]), in_hbm(out_grad[0]), in_hbm(resp_kv[0]), query_bias, kv_bias)
    bias = score(q, g, prefix, kv_bias, own_kv, in_hbm(e), in_hbm(dp), stat)
    part = jnp.sum(exchange(bias, PLANE), 0)
    part, lengths = lax.optimization_barrier((part, lengths))
    att, dq, own_grad, pre = grads(lengths, q, g, prefix, kv_bias, own_kv)
    part = exchange(jnp.broadcast_to(part, (32, 2, HD)), COLUMN)
    pre_grad, qsum, kvsum = finish(exchange(enclose(pre, part), GRP))
    return (
        att[None],
        dq[None],
        own_grad[None],
        pre_grad[None],
        qsum.reshape(QH * HD),
        kvsum.reshape(2 * WIDTH),
    )


def solution(mesh):
    finer = Mesh(mesh.devices.reshape(2, 4, 2, 32, 2), ("grp_0", "grp_1", "grp_2", "dp_0", "dp_1"))
    rows = P(DP, GRP, None)
    return jax.shard_map(
        local,
        mesh=finer,
        in_specs=(rows, rows, rows, P(), P(), rows, P(DP, GRP)),
        out_specs=(rows, rows, rows, rows, P(), P()),
        check_vma=False,
    )
```

```python
import jax
import jax.numpy as jnp
from jax import lax
from jax.experimental import pallas as pl
from jax.experimental.pallas import tpu as pltpu
from jax.sharding import Mesh
from jax.sharding import PartitionSpec as P

QH = 20
KVH = 4
HD = 128
RESP = 128
PRE = 256
KEYS = PRE + RESP
GROUP = QH // KVH
WIDTH = KVH * HD
GW = GROUP * HD
PEERS = 16
ROWS = PRE // PEERS
CHUNK = 2 * KVH * ROWS
FACTOR = HD ** (-0.5)
SCALE = FACTOR * 1.4426950408889634
GRP = ("grp_0", "grp_1", "grp_2")
DP = ("dp_0", "dp_1")
PLANE = ("grp_0", "grp_1", "grp_2", "dp_1")
COLUMN = "dp_0"
NEG_BIG = -1e30
VMEM_LIMIT = 24 * 1024 * 1024
BF16 = jnp.bfloat16
F32 = jnp.float32


def dot(a, b, contract):
    return lax.dot_general(a, b, (contract, ((), ())), preferred_element_type=F32)


def in_three(x):
    high = x.astype(BF16).astype(F32)
    rest = x - high
    middle = rest.astype(BF16).astype(F32)
    return high, middle, rest - middle


def stacked(ref):
    return jnp.concatenate([ref[:, h * HD:(h + 1) * HD] for h in range(GROUP)], 0)


def row_sum(weights, rows):
    parts = jnp.concatenate([*in_three(weights), jnp.zeros((5, weights.shape[1]), F32)], 0)
    return jnp.sum(dot(parts.astype(BF16), rows, ((1,), (0,))), 0, keepdims=True)


def biased(values, bias_ref, index):
    return (values.astype(F32) + bias_ref[pl.ds(index, 1), :]).astype(BF16)


def raw_pair(both, q, g):
    zero = jnp.zeros((RESP, HD), BF16)
    pair = jnp.concatenate([jnp.concatenate([q, zero], 1), jnp.concatenate([zero, g], 1)], 0)
    return dot(both, pair, ((1,), (1,)))


def own_kernel(len_ref, query_ref, grad_ref, k_ref, v_ref, qb_ref, kb_ref,
               q_ref, g_ref, own_ref, e_ref, dp_ref, stat_ref):
    j = pl.program_id(0)
    live = lax.broadcasted_iota(jnp.int32, (RESP, HD), 0) < len_ref[0, 0]
    for h in range(GROUP):
        cols = slice(h * HD, (h + 1) * HD)
        q_ref[:, cols] = biased(query_ref[:, cols], qb_ref, j * GROUP + h)
        g_ref[:, cols] = jnp.where(live, grad_ref[:, cols].astype(F32), 0.0).astype(BF16)
    keys = biased(k_ref[...], kb_ref, j)
    vals = biased(v_ref[...], kb_ref, KVH + j)
    col = pl.multiple_of(j * HD, HD)
    own_ref[:, pl.ds(col, HD)] = keys
    own_ref[:, pl.ds(col + WIDTH, HD)] = vals
    both = jnp.concatenate([keys, vals], 1)
    allow = lax.broadcasted_iota(jnp.int32, (RESP, RESP), 0) <= lax.broadcasted_iota(jnp.int32, (RESP, RESP), 1)
    for h in range(GROUP):
        cols = slice(h * HD, (h + 1) * HD)
        raw = raw_pair(both, q_ref[:, cols], g_ref[:, cols])
        s = jnp.where(allow, raw[:, :RESP], NEG_BIG)
        dp = raw[:, RESP:]
        top = jnp.max(s, 0, keepdims=True)
        e = jnp.exp2((s - top) * SCALE)
        e_ref[:, cols] = e
        dp_ref[:, cols] = dp
        stat_ref[0, 0:1, cols] = top
        stat_ref[0, 1:2, cols] = jnp.sum(e, 0, keepdims=True)
        stat_ref[0, 2:3, cols] = jnp.sum(e * dp, 0, keepdims=True)
        stat_ref[0, 3:8, cols] = jnp.zeros((5, HD), F32)


STEP = 64


def fold(x, how):
    return how(x.reshape(-1, 8, HD), 0)


def score_kernel(q_ref, g_ref, pk_ref, pv_ref, kb_ref, own_ref, e_ref, dp_ref, stat_ref, bias_ref, raw_ref, ds_ref):
    j = pl.program_id(0)
    keys = biased(pk_ref[...], kb_ref, j)
    both = jnp.concatenate([keys, biased(pv_ref[...], kb_ref, KVH + j)], 1)
    for h in range(GROUP):
        cols = slice(h * HD, (h + 1) * HD)
        raw_ref[h] = raw_pair(both, q_ref[:, cols], g_ref[:, cols])
    shift_sums = []
    prob_sums = []
    for h in range(GROUP):
        cols = slice(h * HD, (h + 1) * HD)
        own_top = stat_ref[0, 0:1, cols]
        high = jnp.full((8, HD), NEG_BIG, F32)
        for at in range(0, PRE, STEP):
            high = jnp.maximum(high, fold(raw_ref[h, at:at + STEP, :RESP], jnp.max))
        top = jnp.maximum(own_top, jnp.max(high, 0, keepdims=True))
        total = jnp.zeros((8, HD), F32)
        meet = jnp.zeros((8, HD), F32)
        for at in range(0, PRE, STEP):
            e = jnp.exp2((raw_ref[h, at:at + STEP, :RESP] - top) * SCALE)
            raw_ref[h, at:at + STEP, :RESP] = e
            total = total + fold(e, jnp.sum)
            meet = meet + fold(e * raw_ref[h, at:at + STEP, RESP:], jnp.sum)
        fade = jnp.exp2((own_top - top) * SCALE)
        inverse = 1.0 / (stat_ref[0, 1:2, cols] * fade + jnp.sum(total, 0, keepdims=True))
        row = (stat_ref[0, 2:3, cols] * fade + jnp.sum(meet, 0, keepdims=True)) * inverse
        own_inverse = fade * inverse
        prob_sum = jnp.zeros((8, HD), F32)
        shift_sum = jnp.zeros((8, HD), F32)
        for at in range(0, KEYS, STEP):
            if at < PRE:
                p = raw_ref[h, at:at + STEP, :RESP] * inverse
                dp = raw_ref[h, at:at + STEP, RESP:]
            else:
                p = e_ref[at - PRE:at - PRE + STEP, cols] * own_inverse
                dp = dp_ref[at - PRE:at - PRE + STEP, cols]
            pb = p.astype(BF16)
            dsb = (p * (dp - row)).astype(BF16)
            ds_ref[at:at + STEP, cols] = dsb
            prob_sum = prob_sum + fold(pb.astype(F32), jnp.sum)
            shift_sum = shift_sum + fold(dsb.astype(F32), jnp.sum)
        prob_sums.append(jnp.sum(prob_sum, 0, keepdims=True))
        shift_sums.append(jnp.sum(shift_sum, 0, keepdims=True))

    def put(index, value):
        for copy in range(2):
            bias_ref[pl.ds(2 * (index // 2) + copy, 1), pl.ds(index % 2, 1), :] = value.reshape(1, 1, HD)

    dq = dot(ds_ref[...], jnp.concatenate([keys, own_ref[...]], 0), ((0,), (0,))) * FACTOR
    for h in range(GROUP):
        put(j * GROUP + h, jnp.sum(dq[h * RESP:(h + 1) * RESP], 0, keepdims=True))
    put(QH + j, row_sum(jnp.concatenate(shift_sums, 1), stacked(q_ref)) * FACTOR)
    put(QH + KVH + j, row_sum(jnp.concatenate(prob_sums, 1), stacked(g_ref)))
    put(QH + 2 * KVH + j, jnp.zeros((1, HD), F32))


def grad_kernel(len_ref, q_ref, g_ref, pk_ref, pv_ref, kb_ref, ok_ref, ov_ref,
                att_ref, dq_ref, own_ref, pre_ref, pt_ref, ds_ref):
    j = pl.program_id(0)
    keys = jnp.concatenate([biased(pk_ref[...], kb_ref, j), ok_ref[...]], 0)
    vals = jnp.concatenate([biased(pv_ref[...], kb_ref, KVH + j), ov_ref[...]], 0)
    both = jnp.concatenate([keys, vals], 1)
    allow = lax.broadcasted_iota(jnp.int32, (RESP, RESP), 0) <= lax.broadcasted_iota(jnp.int32, (RESP, RESP), 1)
    for h in range(GROUP):
        cols = slice(h * HD, (h + 1) * HD)
        raw = raw_pair(both, q_ref[:, cols], g_ref[:, cols])
        s = raw[:, :RESP]
        dp = raw[:, RESP:]
        s = jnp.concatenate([s[:PRE], jnp.where(allow, s[PRE:], NEG_BIG)], 0)
        e = jnp.exp2((s - jnp.max(s, 0, keepdims=True)) * SCALE)
        p = e * (1.0 / jnp.sum(e, 0, keepdims=True))
        row = jnp.sum(p * dp, 0, keepdims=True)
        pt_ref[:, cols] = p.astype(BF16)
        ds_ref[:, cols] = (p * (dp - row)).astype(BF16)
    pt = pt_ref[...]
    ds = ds_ref[...]
    dk = dot(ds, stacked(q_ref), ((1,), (0,))) * FACTOR
    dv = dot(pt, stacked(g_ref), ((1,), (0,)))
    col = pl.multiple_of(j * HD, HD)
    own_ref[:, pl.ds(col, HD)] = dk[PRE:].astype(BF16)
    own_ref[:, pl.ds(col + WIDTH, HD)] = dv[PRE:].astype(BF16)
    at = pl.multiple_of(j * ROWS, ROWS)
    pre_ref[:, pl.ds(at, ROWS), :] = dk[:PRE].astype(BF16).reshape(PEERS, ROWS, HD)
    pre_ref[:, pl.ds(at + KVH * ROWS, ROWS), :] = dv[:PRE].astype(BF16).reshape(PEERS, ROWS, HD)
    dq = dot(ds, keys, ((0,), (0,))) * FACTOR
    out = dot(pt, vals, ((0,), (0,)))
    live = lax.broadcasted_iota(jnp.int32, (RESP, HD), 0) < len_ref[0, 0]
    for h in range(GROUP):
        cols = slice(h * HD, (h + 1) * HD)
        rows = slice(h * RESP, (h + 1) * RESP)
        att_ref[:, cols] = jnp.where(live, out[rows], 0.0).astype(BF16)
        dq_ref[:, cols] = dq[rows].astype(BF16)


def enclose_kernel(buffer_ref, parts_ref, out_ref):
    del buffer_ref
    total = jnp.sum(parts_ref[...], 0)
    rows = jnp.concatenate([*in_three(total), jnp.zeros((2, HD), F32)], 0).astype(BF16)
    out_ref[...] = jnp.broadcast_to(rows[None], (PEERS, 8, HD))


def finish_kernel(arrived_ref, pre_ref, q_ref, kv_ref):
    for m in range(2 * KVH):
        piece = arrived_ref[:, m * ROWS:(m + 1) * ROWS, :].astype(F32)
        pre_ref[:, m * HD:(m + 1) * HD] = jnp.sum(piece, 0).astype(BF16)
    for i in range((QH + 2 * KVH) // 2):
        tail = arrived_ref[i, CHUNK:, :].astype(F32)
        pair = tail[0:2] + tail[2:4] + tail[4:6]
        if 2 * i < QH:
            q_ref[2 * i:2 * i + 2, :] = pair
        else:
            kv_ref[2 * i - QH:2 * i - QH + 2, :] = pair


def first(j):
    return 0, j


def second(j):
    return 0, KVH + j


def whole(j):
    return 0, 0


def params():
    return pltpu.CompilerParams(dimension_semantics=("arbitrary",), vmem_limit_bytes=VMEM_LIMIT)


def cost(matmuls):
    return pl.CostEstimate(
        flops=matmuls * 2 * QH * RESP * KEYS * HD, bytes_accessed=4_000_000, transcendentals=QH * RESP * KEYS
    )


def own(length, query, out_grad, resp_kv, query_bias, kv_bias):
    wide = pl.BlockSpec((RESP, GW), first)
    return pl.pallas_call(
        own_kernel,
        grid=(KVH,),
        in_specs=[
            pl.BlockSpec(memory_space=pltpu.SMEM),
            wide,
            wide,
            pl.BlockSpec((RESP, HD), first),
            pl.BlockSpec((RESP, HD), second),
            pl.BlockSpec((QH, HD), whole),
            pl.BlockSpec((2 * KVH, HD), whole),
        ],
        out_specs=[
            wide,
            wide,
            pl.BlockSpec((RESP, 2 * WIDTH), lambda j: (0, 0)),
            wide,
            wide,
            pl.BlockSpec((1, 8, GW), lambda j: (j, 0, 0)),
        ],
        out_shape=[
            jax.ShapeDtypeStruct((RESP, QH * HD), BF16),
            jax.ShapeDtypeStruct((RESP, QH * HD), BF16),
            jax.ShapeDtypeStruct((RESP, 2 * WIDTH), BF16),
            pltpu.HBM((RESP, QH * HD), F32),
            pltpu.HBM((RESP, QH * HD), F32),
            jax.ShapeDtypeStruct((KVH, 8, GW), F32),
        ],
        compiler_params=params(),
        cost_estimate=cost(1),
        name="own",
    )(length, query, out_grad, resp_kv, resp_kv, query_bias, kv_bias)


def score(q, g, prefix, kv_bias, own_kv, e, dp, stat):
    wide = pl.BlockSpec((RESP, GW), first)
    return pl.pallas_call(
        score_kernel,
        grid=(KVH,),
        in_specs=[
            wide,
            wide,
            pl.BlockSpec((PRE, HD), first),
            pl.BlockSpec((PRE, HD), second),
            pl.BlockSpec((2 * KVH, HD), whole),
            pl.BlockSpec((RESP, HD), first),
            wide,
            wide,
            pl.BlockSpec((1, 8, GW), lambda j: (j, 0, 0)),
        ],
        out_specs=pl.BlockSpec((32, 2, HD), lambda j: (0, 0, 0)),
        out_shape=jax.ShapeDtypeStruct((32, 2, HD), F32),
        scratch_shapes=[pltpu.VMEM((GROUP, PRE, 2 * RESP), F32), pltpu.VMEM((KEYS, GW), BF16)],
        compiler_params=params(),
        cost_estimate=cost(3),
        name="score",
    )(q, g, prefix, prefix, kv_bias, own_kv, e, dp, stat)


def grads(length, q, g, prefix, kv_bias, own_kv):
    wide = pl.BlockSpec((RESP, GW), first)
    return pl.pallas_call(
        grad_kernel,
        grid=(KVH,),
        in_specs=[
            pl.BlockSpec(memory_space=pltpu.SMEM),
            wide,
            wide,
            pl.BlockSpec((PRE, HD), first),
            pl.BlockSpec((PRE, HD), second),
            pl.BlockSpec((2 * KVH, HD), whole),
            pl.BlockSpec((RESP, HD), first),
            pl.BlockSpec((RESP, HD), second),
        ],
        out_specs=[
            wide,
            wide,
            pl.BlockSpec((RESP, 2 * WIDTH), whole),
            pl.BlockSpec((PEERS, CHUNK + 8, HD), lambda j: (0, 0, 0)),
        ],
        out_shape=[
            jax.ShapeDtypeStruct((RESP, QH * HD), BF16),
            jax.ShapeDtypeStruct((RESP, QH * HD), BF16),
            jax.ShapeDtypeStruct((RESP, 2 * WIDTH), BF16),
            jax.ShapeDtypeStruct((PEERS, CHUNK + 8, HD), BF16),
        ],
        scratch_shapes=[pltpu.VMEM((KEYS, GW), BF16), pltpu.VMEM((KEYS, GW), BF16)],
        compiler_params=params(),
        cost_estimate=cost(6),
        name="grads",
    )(length, q, g, prefix, prefix, kv_bias, own_kv, own_kv)


def enclose(pre, parts):
    return pl.pallas_call(
        enclose_kernel,
        grid=(1,),
        in_specs=[pl.BlockSpec(memory_space=pl.ANY), pl.BlockSpec((32, 2, HD), lambda i: (0, 0, 0))],
        out_specs=pl.BlockSpec((PEERS, 8, HD), lambda i: (0, CHUNK // 8, 0)),
        out_shape=jax.ShapeDtypeStruct(pre.shape, BF16),
        input_output_aliases={0: 0},
        compiler_params=params(),
        name="enclose",
    )(pre, parts)


def finish(arrived):
    return pl.pallas_call(
        finish_kernel,
        out_shape=[
            jax.ShapeDtypeStruct((ROWS, 2 * WIDTH), BF16),
            jax.ShapeDtypeStruct((QH, HD), F32),
            jax.ShapeDtypeStruct((2 * KVH, HD), F32),
        ],
        compiler_params=pltpu.CompilerParams(vmem_limit_bytes=VMEM_LIMIT),
        name="finish",
    )(arrived)


def in_hbm(x):
    return pltpu.with_memory_space_constraint(x, pltpu.HBM)


def exchange(pieces, axes):
    return lax.all_to_all(pieces, axes, 0, 0, tiled=True)


def local(query, resp_kv, prefix_kv, query_bias, kv_bias, out_grad, lengths):
    query_bias = query_bias.reshape(QH, HD)
    kv_bias = kv_bias.reshape(2 * KVH, HD)
    prefix = exchange(jnp.broadcast_to(prefix_kv[0], (PEERS, ROWS, 2 * WIDTH)), GRP).reshape(PRE, 2 * WIDTH)
    q, g, own_kv, e, dp, stat = own(lengths, in_hbm(query[0]), in_hbm(out_grad[0]), in_hbm(resp_kv[0]), query_bias, kv_bias)
    bias = score(q, g, prefix, kv_bias, own_kv, in_hbm(e), in_hbm(dp), stat)
    part = jnp.sum(exchange(bias, PLANE), 0)
    part, lengths = lax.optimization_barrier((part, lengths))
    att, dq, own_grad, pre = grads(lengths, q, g, prefix, kv_bias, own_kv)
    order = [(i + 20) % 32 for i in range(32)]
    part = lax.all_to_all(
        jnp.broadcast_to(part, (32, 2, HD)), COLUMN, 0, 0, axis_index_groups=[order], tiled=True
    )
    pre_grad, qsum, kvsum = finish(exchange(enclose(pre, part), GRP))
    return (
        att[None],
        dq[None],
        own_grad[None],
        pre_grad[None],
        qsum.reshape(QH * HD),
        kvsum.reshape(2 * WIDTH),
    )


def solution(mesh):
    finer = Mesh(mesh.devices.reshape(2, 4, 2, 32, 2), ("grp_0", "grp_1", "grp_2", "dp_0", "dp_1"))
    rows = P(DP, GRP, None)
    return jax.shard_map(
        local,
        mesh=finer,
        in_specs=(rows, rows, rows, P(), P(), rows, P(DP, GRP)),
        out_specs=(rows, rows, rows, rows, P(), P()),
        check_vma=False,
    )
```

```python
import functools

import jax
import jax.numpy as jnp
from jax import lax
from jax.experimental import pallas as pl
from jax.experimental.pallas import tpu as pltpu
from jax.sharding import Mesh
from jax.sharding import PartitionSpec as P

QH = 20
KVH = 4
HD = 128
RESP = 128
PRE = 256
KEYS = PRE + RESP
GROUP = QH // KVH
WIDTH = KVH * HD
GW = GROUP * HD
PEERS = 16
ROWS = PRE // PEERS
CHUNK = 2 * KVH * ROWS
FACTOR = HD ** (-0.5)
SCALE = FACTOR * 1.4426950408889634
GRP = ("grp_0", "grp_1", "grp_2")
DP = ("dp_0", "dp_1")
PLANE = ("grp_0", "grp_1", "grp_2", "dp_1")
COLUMN = "dp_0"
NEG_BIG = -1e30
FIRST = 2
VMEM_LIMIT = 24 * 1024 * 1024
BF16 = jnp.bfloat16
F32 = jnp.float32


def dot(a, b, contract):
    return lax.dot_general(a, b, (contract, ((), ())), preferred_element_type=F32)


def in_three(x):
    high = x.astype(BF16).astype(F32)
    rest = x - high
    middle = rest.astype(BF16).astype(F32)
    return high, middle, rest - middle


def stacked(ref):
    return jnp.concatenate([ref[:, h * HD:(h + 1) * HD] for h in range(GROUP)], 0)


def row_sum(weights, rows):
    parts = jnp.concatenate([*in_three(weights), jnp.zeros((5, weights.shape[1]), F32)], 0)
    return jnp.sum(dot(parts.astype(BF16), rows, ((1,), (0,))), 0, keepdims=True)


def biased(values, bias_ref, index):
    return (values.astype(F32) + bias_ref[pl.ds(index, 1), :]).astype(BF16)


def raw_pair(both, q, g):
    zero = jnp.zeros((RESP, HD), BF16)
    pair = jnp.concatenate([jnp.concatenate([q, zero], 1), jnp.concatenate([zero, g], 1)], 0)
    return dot(both, pair, ((1,), (1,)))


def own_kernel(len_ref, query_ref, grad_ref, k_ref, v_ref, qb_ref, kb_ref,
               q_ref, g_ref, own_ref, e_ref, dp_ref, stat_ref):
    j = pl.program_id(0)
    live = lax.broadcasted_iota(jnp.int32, (RESP, HD), 0) < len_ref[0, 0]
    for h in range(GROUP):
        cols = slice(h * HD, (h + 1) * HD)
        q_ref[:, cols] = biased(query_ref[:, cols], qb_ref, j * GROUP + h)
        g_ref[:, cols] = jnp.where(live, grad_ref[:, cols].astype(F32), 0.0).astype(BF16)
    keys = biased(k_ref[...], kb_ref, j)
    vals = biased(v_ref[...], kb_ref, KVH + j)
    col = pl.multiple_of(j * HD, HD)
    own_ref[:, pl.ds(col, HD)] = keys
    own_ref[:, pl.ds(col + WIDTH, HD)] = vals
    both = jnp.concatenate([keys, vals], 1)
    allow = lax.broadcasted_iota(jnp.int32, (RESP, RESP), 0) <= lax.broadcasted_iota(jnp.int32, (RESP, RESP), 1)
    for h in range(GROUP):
        cols = slice(h * HD, (h + 1) * HD)
        raw = raw_pair(both, q_ref[:, cols], g_ref[:, cols])
        s = jnp.where(allow, raw[:, :RESP], NEG_BIG)
        dp = raw[:, RESP:]
        top = jnp.max(s, 0, keepdims=True)
        e = jnp.exp2((s - top) * SCALE)
        e_ref[:, cols] = e
        dp_ref[:, cols] = dp
        stat_ref[0, 0:1, cols] = top
        stat_ref[0, 1:2, cols] = jnp.sum(e, 0, keepdims=True)
        stat_ref[0, 2:3, cols] = jnp.sum(e * dp, 0, keepdims=True)
        stat_ref[0, 3:8, cols] = jnp.zeros((5, HD), F32)


STEP = 64


def fold(x, how):
    return how(x.reshape(-1, 8, HD), 0)


def score_kernel(q_ref, g_ref, pk_ref, pv_ref, kb_ref, own_ref, e_ref, dp_ref, stat_ref, bias_ref, raw_ref, ds_ref):
    j = pl.program_id(0)
    keys = biased(pk_ref[...], kb_ref, j)
    both = jnp.concatenate([keys, biased(pv_ref[...], kb_ref, KVH + j)], 1)
    for h in range(GROUP):
        cols = slice(h * HD, (h + 1) * HD)
        raw_ref[h] = raw_pair(both, q_ref[:, cols], g_ref[:, cols])
    all_keys = jnp.concatenate([keys, own_ref[...]], 0)
    ones = jnp.ones((8, RESP), BF16)
    key_weights = []
    key_sum = jnp.zeros((1, HD), F32)
    value_sum = jnp.zeros((1, HD), F32)
    for h in range(GROUP):
        cols = slice(h * HD, (h + 1) * HD)
        own_top = stat_ref[0, 0:1, cols]
        high = jnp.full((8, HD), NEG_BIG, F32)
        for at in range(0, PRE, STEP):
            high = jnp.maximum(high, fold(raw_ref[h, at:at + STEP, :RESP], jnp.max))
        top = jnp.maximum(own_top, jnp.max(high, 0, keepdims=True))
        total = jnp.zeros((8, HD), F32)
        meet = jnp.zeros((8, HD), F32)
        for at in range(0, PRE, STEP):
            e = jnp.exp2((raw_ref[h, at:at + STEP, :RESP] - top) * SCALE)
            raw_ref[h, at:at + STEP, :RESP] = e
            total = total + fold(e, jnp.sum)
            meet = meet + fold(e * raw_ref[h, at:at + STEP, RESP:], jnp.sum)
        fade = jnp.exp2((own_top - top) * SCALE)
        inverse = 1.0 / (stat_ref[0, 1:2, cols] * fade + jnp.sum(total, 0, keepdims=True))
        row = (stat_ref[0, 2:3, cols] * fade + jnp.sum(meet, 0, keepdims=True)) * inverse
        own_inverse = fade * inverse
        prob_sum = jnp.zeros((8, HD), F32)
        shift_sum = jnp.zeros((8, HD), F32)
        for at in range(0, KEYS, STEP):
            if at < PRE:
                p = raw_ref[h, at:at + STEP, :RESP] * inverse
                dp = raw_ref[h, at:at + STEP, RESP:]
            else:
                p = e_ref[at - PRE:at - PRE + STEP, cols] * own_inverse
                dp = dp_ref[at - PRE:at - PRE + STEP, cols]
            pb = p.astype(BF16)
            dsb = (p * (dp - row)).astype(BF16)
            ds_ref[at:at + STEP, cols] = dsb
            prob_sum = prob_sum + fold(pb.astype(F32), jnp.sum)
            shift_sum = shift_sum + fold(dsb.astype(F32), jnp.sum)
        key_weights.append(dot(ones, ds_ref[:, cols], ((1,), (1,)))[0:1])
        key_sum = key_sum + row_sum(jnp.sum(shift_sum, 0, keepdims=True), q_ref[:, cols])
        value_sum = value_sum + row_sum(jnp.sum(prob_sum, 0, keepdims=True), g_ref[:, cols])

    def put(index, value):
        for copy in range(2):
            bias_ref[pl.ds(2 * (index // 2) + copy, 1), pl.ds(index % 2, 1), :] = value.reshape(1, 1, HD)

    parts = [*in_three(jnp.concatenate(key_weights, 0)), jnp.zeros((1, KEYS), F32)]
    query_sum = dot(jnp.concatenate(parts, 0).astype(BF16), all_keys, ((1,), (0,)))
    for h in range(GROUP):
        mine = query_sum[h:h + 1] + query_sum[GROUP + h:GROUP + h + 1] + query_sum[2 * GROUP + h:2 * GROUP + h + 1]
        put(j * GROUP + h, mine * FACTOR)
    put(QH + j, key_sum * FACTOR)
    put(QH + KVH + j, value_sum)
    put(QH + 2 * KVH + j, jnp.zeros((1, HD), F32))


def grad_kernel(base, len_ref, q_ref, g_ref, pk_ref, pv_ref, kb_ref, ok_ref, ov_ref, *rest):
    *before, att_ref, dq_ref, own_ref, pre_ref, pt_ref, ds_ref = rest
    j = base + pl.program_id(0)
    if before:

        @pl.when(j == base)
        def _():
            own_ref[...] = before[2][...]
            pre_ref[...] = before[3][...]

    keys = jnp.concatenate([biased(pk_ref[...], kb_ref, j), ok_ref[...]], 0)
    vals = jnp.concatenate([biased(pv_ref[...], kb_ref, KVH + j), ov_ref[...]], 0)
    both = jnp.concatenate([keys, vals], 1)
    allow = lax.broadcasted_iota(jnp.int32, (RESP, RESP), 0) <= lax.broadcasted_iota(jnp.int32, (RESP, RESP), 1)
    for h in range(GROUP):
        cols = slice(h * HD, (h + 1) * HD)
        raw = raw_pair(both, q_ref[:, cols], g_ref[:, cols])
        s = raw[:, :RESP]
        dp = raw[:, RESP:]
        s = jnp.concatenate([s[:PRE], jnp.where(allow, s[PRE:], NEG_BIG)], 0)
        e = jnp.exp2((s - jnp.max(s, 0, keepdims=True)) * SCALE)
        p = e * (1.0 / jnp.sum(e, 0, keepdims=True))
        row = jnp.sum(p * dp, 0, keepdims=True)
        pt_ref[:, cols] = p.astype(BF16)
        ds_ref[:, cols] = (p * (dp - row)).astype(BF16)
    pt = pt_ref[...]
    ds = ds_ref[...]
    dk = dot(ds, stacked(q_ref), ((1,), (0,))) * FACTOR
    dv = dot(pt, stacked(g_ref), ((1,), (0,)))
    col = pl.multiple_of(j * HD, HD)
    own_ref[:, pl.ds(col, HD)] = dk[PRE:].astype(BF16)
    own_ref[:, pl.ds(col + WIDTH, HD)] = dv[PRE:].astype(BF16)
    at = pl.multiple_of(j * ROWS, ROWS)
    pre_ref[:, pl.ds(at, ROWS), :] = dk[:PRE].astype(BF16).reshape(PEERS, ROWS, HD)
    pre_ref[:, pl.ds(at + KVH * ROWS, ROWS), :] = dv[:PRE].astype(BF16).reshape(PEERS, ROWS, HD)
    dq = dot(ds, keys, ((0,), (0,))) * FACTOR
    out = dot(pt, vals, ((0,), (0,)))
    live = lax.broadcasted_iota(jnp.int32, (RESP, HD), 0) < len_ref[0, 0]
    for h in range(GROUP):
        cols = slice(h * HD, (h + 1) * HD)
        rows = slice(h * RESP, (h + 1) * RESP)
        att_ref[:, cols] = jnp.where(live, out[rows], 0.0).astype(BF16)
        dq_ref[:, cols] = dq[rows].astype(BF16)


def enclose_kernel(buffer_ref, parts_ref, out_ref):
    del buffer_ref
    total = jnp.sum(parts_ref[...], 0)
    rows = jnp.concatenate([*in_three(total), jnp.zeros((2, HD), F32)], 0).astype(BF16)
    out_ref[...] = jnp.broadcast_to(rows[None], (PEERS, 8, HD))


def finish_kernel(arrived_ref, pre_ref, q_ref, kv_ref):
    for m in range(2 * KVH):
        piece = arrived_ref[:, m * ROWS:(m + 1) * ROWS, :].astype(F32)
        pre_ref[:, m * HD:(m + 1) * HD] = jnp.sum(piece, 0).astype(BF16)
    for i in range((QH + 2 * KVH) // 2):
        tail = arrived_ref[i, CHUNK:, :].astype(F32)
        pair = tail[0:2] + tail[2:4] + tail[4:6]
        if 2 * i < QH:
            q_ref[2 * i:2 * i + 2, :] = pair
        else:
            kv_ref[2 * i - QH:2 * i - QH + 2, :] = pair


def first(j):
    return 0, j


def second(j):
    return 0, KVH + j


def whole(j):
    return 0, 0


def params():
    return pltpu.CompilerParams(dimension_semantics=("arbitrary",), vmem_limit_bytes=VMEM_LIMIT)


def cost(matmuls):
    return pl.CostEstimate(
        flops=int(matmuls * 2 * QH * RESP * KEYS * HD), bytes_accessed=4_000_000, transcendentals=QH * RESP * KEYS
    )


def own(length, query, out_grad, resp_kv, query_bias, kv_bias):
    wide = pl.BlockSpec((RESP, GW), first)
    return pl.pallas_call(
        own_kernel,
        grid=(KVH,),
        in_specs=[
            pl.BlockSpec(memory_space=pltpu.SMEM),
            wide,
            wide,
            pl.BlockSpec((RESP, HD), first),
            pl.BlockSpec((RESP, HD), second),
            pl.BlockSpec((QH, HD), whole),
            pl.BlockSpec((2 * KVH, HD), whole),
        ],
        out_specs=[
            wide,
            wide,
            pl.BlockSpec((RESP, 2 * WIDTH), lambda j: (0, 0)),
            wide,
            wide,
            pl.BlockSpec((1, 8, GW), lambda j: (j, 0, 0)),
        ],
        out_shape=[
            jax.ShapeDtypeStruct((RESP, QH * HD), BF16),
            jax.ShapeDtypeStruct((RESP, QH * HD), BF16),
            jax.ShapeDtypeStruct((RESP, 2 * WIDTH), BF16),
            pltpu.HBM((RESP, QH * HD), F32),
            pltpu.HBM((RESP, QH * HD), F32),
            jax.ShapeDtypeStruct((KVH, 8, GW), F32),
        ],
        compiler_params=params(),
        cost_estimate=cost(1),
        name="own",
    )(length, query, out_grad, resp_kv, resp_kv, query_bias, kv_bias)


def score(q, g, prefix, kv_bias, own_kv, e, dp, stat):
    wide = pl.BlockSpec((RESP, GW), first)
    return pl.pallas_call(
        score_kernel,
        grid=(KVH,),
        in_specs=[
            wide,
            wide,
            pl.BlockSpec((PRE, HD), first),
            pl.BlockSpec((PRE, HD), second),
            pl.BlockSpec((2 * KVH, HD), whole),
            pl.BlockSpec((RESP, HD), first),
            wide,
            wide,
            pl.BlockSpec((1, 8, GW), lambda j: (j, 0, 0)),
        ],
        out_specs=pl.BlockSpec((32, 2, HD), lambda j: (0, 0, 0)),
        out_shape=jax.ShapeDtypeStruct((32, 2, HD), F32),
        scratch_shapes=[pltpu.VMEM((GROUP, PRE, 2 * RESP), F32), pltpu.VMEM((KEYS, GW), BF16)],
        compiler_params=params(),
        cost_estimate=cost(3),
        name="score",
    )(q, g, prefix, prefix, kv_bias, own_kv, e, dp, stat)


def grads(base, count, length, q, g, prefix, kv_bias, own_kv, *results):
    def low(j):
        return 0, base + j

    def high(j):
        return 0, KVH + base + j

    wide = pl.BlockSpec((RESP, GW), low)
    rest = [
        pl.BlockSpec((RESP, 2 * WIDTH), whole),
        pl.BlockSpec((PEERS, CHUNK + 8, HD), lambda j: (0, 0, 0)),
    ]
    anywhere = pl.BlockSpec(memory_space=pl.ANY)
    return pl.pallas_call(
        functools.partial(grad_kernel, base),
        grid=(count,),
        in_specs=[
            pl.BlockSpec(memory_space=pltpu.SMEM),
            wide,
            wide,
            pl.BlockSpec((PRE, HD), low),
            pl.BlockSpec((PRE, HD), high),
            pl.BlockSpec((2 * KVH, HD), whole),
            pl.BlockSpec((RESP, HD), low),
            pl.BlockSpec((RESP, HD), high),
            *([anywhere, anywhere, *rest] if results else []),
        ],
        out_specs=[wide, wide, *rest],
        out_shape=[
            jax.ShapeDtypeStruct((RESP, QH * HD), BF16),
            jax.ShapeDtypeStruct((RESP, QH * HD), BF16),
            jax.ShapeDtypeStruct((RESP, 2 * WIDTH), BF16),
            jax.ShapeDtypeStruct((PEERS, CHUNK + 8, HD), BF16),
        ],
        scratch_shapes=[pltpu.VMEM((KEYS, GW), BF16), pltpu.VMEM((KEYS, GW), BF16)],
        input_output_aliases={8: 0, 9: 1} if results else {},
        compiler_params=params(),
        cost_estimate=cost(6 * count / KVH),
        name="grads",
    )(length, q, g, prefix, prefix, kv_bias, own_kv, own_kv, *results)


def enclose(pre, parts):
    return pl.pallas_call(
        enclose_kernel,
        grid=(1,),
        in_specs=[pl.BlockSpec(memory_space=pl.ANY), pl.BlockSpec((32, 2, HD), lambda i: (0, 0, 0))],
        out_specs=pl.BlockSpec((PEERS, 8, HD), lambda i: (0, CHUNK // 8, 0)),
        out_shape=jax.ShapeDtypeStruct(pre.shape, BF16),
        input_output_aliases={0: 0},
        compiler_params=params(),
        name="enclose",
    )(pre, parts)


def finish(arrived):
    return pl.pallas_call(
        finish_kernel,
        out_shape=[
            jax.ShapeDtypeStruct((ROWS, 2 * WIDTH), BF16),
            jax.ShapeDtypeStruct((QH, HD), F32),
            jax.ShapeDtypeStruct((2 * KVH, HD), F32),
        ],
        compiler_params=pltpu.CompilerParams(vmem_limit_bytes=VMEM_LIMIT),
        name="finish",
    )(arrived)


def in_hbm(x):
    return pltpu.with_memory_space_constraint(x, pltpu.HBM)


def exchange(pieces, axes):
    return lax.all_to_all(pieces, axes, 0, 0, tiled=True)


def local(query, resp_kv, prefix_kv, query_bias, kv_bias, out_grad, lengths):
    query_bias = query_bias.reshape(QH, HD)
    kv_bias = kv_bias.reshape(2 * KVH, HD)
    prefix = exchange(jnp.broadcast_to(prefix_kv[0], (PEERS, ROWS, 2 * WIDTH)), GRP).reshape(PRE, 2 * WIDTH)
    q, g, own_kv, e, dp, stat = own(lengths, in_hbm(query[0]), in_hbm(out_grad[0]), in_hbm(resp_kv[0]), query_bias, kv_bias)
    bias = score(q, g, prefix, kv_bias, own_kv, in_hbm(e), in_hbm(dp), stat)
    part = jnp.sum(exchange(bias, PLANE), 0)
    results = grads(0, FIRST, lengths, q, g, prefix, kv_bias, own_kv)
    part, lengths, results = lax.optimization_barrier((part, lengths, results))
    att, dq, own_grad, pre = grads(FIRST, KVH - FIRST, lengths, q, g, prefix, kv_bias, own_kv, *results)
    order = [(i + 20) % 32 for i in range(32)]
    part = lax.all_to_all(
        jnp.broadcast_to(part, (32, 2, HD)), COLUMN, 0, 0, axis_index_groups=[order], tiled=True
    )
    pre_grad, qsum, kvsum = finish(exchange(enclose(pre, part), GRP))
    return (
        att[None],
        dq[None],
        own_grad[None],
        pre_grad[None],
        qsum.reshape(QH * HD),
        kvsum.reshape(2 * WIDTH),
    )


def solution(mesh):
    finer = Mesh(mesh.devices.reshape(2, 4, 2, 32, 2), ("grp_0", "grp_1", "grp_2", "dp_0", "dp_1"))
    rows = P(DP, GRP, None)
    return jax.shard_map(
        local,
        mesh=finer,
        in_specs=(rows, rows, rows, P(), P(), rows, P(DP, GRP)),
        out_specs=(rows, rows, rows, rows, P(), P()),
        check_vma=False,
    )
```

```python
import jax
import jax.numpy as jnp
from jax import lax
from jax.experimental import pallas as pl
from jax.experimental.pallas import tpu as pltpu
from jax.sharding import Mesh
from jax.sharding import PartitionSpec as P

QH = 20
KVH = 4
HD = 128
RESP = 128
PRE = 256
KEYS = PRE + RESP
GROUP = QH // KVH
WIDTH = KVH * HD
GW = GROUP * HD
PEERS = 16
ROWS = PRE // PEERS
CHUNK = 2 * KVH * ROWS
FACTOR = HD ** (-0.5)
SCALE = FACTOR * 1.4426950408889634
GRP = ("grp_0", "grp_1", "grp_2")
DP = ("dp_0", "dp_1")
PLANE = ("grp_0", "grp_1", "grp_2", "dp_1")
COLUMN = "dp_0"
NEG_BIG = -1e30
VMEM_LIMIT = 24 * 1024 * 1024
BF16 = jnp.bfloat16
F32 = jnp.float32


def dot(a, b, contract):
    return lax.dot_general(a, b, (contract, ((), ())), preferred_element_type=F32)


def in_three(x):
    high = x.astype(BF16).astype(F32)
    rest = x - high
    middle = rest.astype(BF16).astype(F32)
    return high, middle, rest - middle


def stacked(ref):
    return jnp.concatenate([ref[:, h * HD:(h + 1) * HD] for h in range(GROUP)], 0)


def row_sum(weights, rows):
    parts = jnp.concatenate([*in_three(weights), jnp.zeros((5, weights.shape[1]), F32)], 0)
    return jnp.sum(dot(parts.astype(BF16), rows, ((1,), (0,))), 0, keepdims=True)


def biased(values, bias_ref, index):
    return (values.astype(F32) + bias_ref[pl.ds(index, 1), :]).astype(BF16)


def raw_pair(both, q, g):
    zero = jnp.zeros((RESP, HD), BF16)
    pair = jnp.concatenate([jnp.concatenate([q, zero], 1), jnp.concatenate([zero, g], 1)], 0)
    return dot(both, pair, ((1,), (1,)))


def own_kernel(len_ref, query_ref, grad_ref, k_ref, v_ref, qb_ref, kb_ref,
               q_ref, g_ref, own_ref, e_ref, dp_ref, stat_ref):
    j = pl.program_id(0)
    live = lax.broadcasted_iota(jnp.int32, (RESP, HD), 0) < len_ref[0, 0]
    for h in range(GROUP):
        cols = slice(h * HD, (h + 1) * HD)
        q_ref[:, cols] = biased(query_ref[:, cols], qb_ref, j * GROUP + h)
        g_ref[:, cols] = jnp.where(live, grad_ref[:, cols].astype(F32), 0.0).astype(BF16)
    keys = biased(k_ref[...], kb_ref, j)
    vals = biased(v_ref[...], kb_ref, KVH + j)
    col = pl.multiple_of(j * HD, HD)
    own_ref[:, pl.ds(col, HD)] = keys
    own_ref[:, pl.ds(col + WIDTH, HD)] = vals
    both = jnp.concatenate([keys, vals], 1)
    allow = lax.broadcasted_iota(jnp.int32, (RESP, RESP), 0) <= lax.broadcasted_iota(jnp.int32, (RESP, RESP), 1)
    for h in range(GROUP):
        cols = slice(h * HD, (h + 1) * HD)
        raw = raw_pair(both, q_ref[:, cols], g_ref[:, cols])
        s = jnp.where(allow, raw[:, :RESP], NEG_BIG)
        dp = raw[:, RESP:]
        top = jnp.max(s, 0, keepdims=True)
        e = jnp.exp2((s - top) * SCALE)
        e_ref[:, cols] = e
        dp_ref[:, cols] = dp
        stat_ref[0, 0:1, cols] = top
        stat_ref[0, 1:2, cols] = jnp.sum(e, 0, keepdims=True)
        stat_ref[0, 2:3, cols] = jnp.sum(e * dp, 0, keepdims=True)
        stat_ref[0, 3:8, cols] = jnp.zeros((5, HD), F32)


STEP = 64


def fold(x, how):
    return how(x.reshape(-1, 8, HD), 0)


def score_kernel(q_ref, g_ref, pk_ref, pv_ref, kb_ref, own_ref, e_ref, dp_ref, stat_ref, bias_ref, raw_ref, ds_ref):
    j = pl.program_id(0)
    keys = biased(pk_ref[...], kb_ref, j)
    both = jnp.concatenate([keys, biased(pv_ref[...], kb_ref, KVH + j)], 1)
    for h in range(GROUP):
        cols = slice(h * HD, (h + 1) * HD)
        raw_ref[h] = raw_pair(both, q_ref[:, cols], g_ref[:, cols])
    shift_sums = []
    prob_sums = []
    for h in range(GROUP):
        cols = slice(h * HD, (h + 1) * HD)
        own_top = stat_ref[0, 0:1, cols]
        high = jnp.full((8, HD), NEG_BIG, F32)
        for at in range(0, PRE, STEP):
            high = jnp.maximum(high, fold(raw_ref[h, at:at + STEP, :RESP], jnp.max))
        top = jnp.maximum(own_top, jnp.max(high, 0, keepdims=True))
        total = jnp.zeros((8, HD), F32)
        meet = jnp.zeros((8, HD), F32)
        for at in range(0, PRE, STEP):
            e = jnp.exp2((raw_ref[h, at:at + STEP, :RESP] - top) * SCALE)
            raw_ref[h, at:at + STEP, :RESP] = e
            total = total + fold(e, jnp.sum)
            meet = meet + fold(e * raw_ref[h, at:at + STEP, RESP:], jnp.sum)
        fade = jnp.exp2((own_top - top) * SCALE)
        inverse = 1.0 / (stat_ref[0, 1:2, cols] * fade + jnp.sum(total, 0, keepdims=True))
        row = (stat_ref[0, 2:3, cols] * fade + jnp.sum(meet, 0, keepdims=True)) * inverse
        own_inverse = fade * inverse
        prob_sum = jnp.zeros((8, HD), F32)
        shift_sum = jnp.zeros((8, HD), F32)
        for at in range(0, KEYS, STEP):
            if at < PRE:
                p = raw_ref[h, at:at + STEP, :RESP] * inverse
                dp = raw_ref[h, at:at + STEP, RESP:]
            else:
                p = e_ref[at - PRE:at - PRE + STEP, cols] * own_inverse
                dp = dp_ref[at - PRE:at - PRE + STEP, cols]
            pb = p.astype(BF16)
            dsb = (p * (dp - row)).astype(BF16)
            ds_ref[at:at + STEP, cols] = dsb
            prob_sum = prob_sum + fold(pb.astype(F32), jnp.sum)
            shift_sum = shift_sum + fold(dsb.astype(F32), jnp.sum)
        prob_sums.append(jnp.sum(prob_sum, 0, keepdims=True))
        shift_sums.append(jnp.sum(shift_sum, 0, keepdims=True))

    def put(index, value):
        for copy in range(2):
            bias_ref[pl.ds(2 * (index // 2) + copy, 1), pl.ds(index % 2, 1), :] = value.reshape(1, 1, HD)

    dq = dot(ds_ref[...], jnp.concatenate([keys, own_ref[...]], 0), ((0,), (0,))) * FACTOR
    for h in range(GROUP):
        put(j * GROUP + h, jnp.sum(dq[h * RESP:(h + 1) * RESP], 0, keepdims=True))
    put(QH + j, row_sum(jnp.concatenate(shift_sums, 1), stacked(q_ref)) * FACTOR)
    put(QH + KVH + j, row_sum(jnp.concatenate(prob_sums, 1), stacked(g_ref)))
    put(QH + 2 * KVH + j, jnp.zeros((1, HD), F32))


def grad_kernel(len_ref, q_ref, g_ref, pk_ref, pv_ref, kb_ref, ok_ref, ov_ref,
                att_ref, dq_ref, own_ref, pre_ref, pt_ref, ds_ref):
    j = pl.program_id(0)
    keys = jnp.concatenate([biased(pk_ref[...], kb_ref, j), ok_ref[...]], 0)
    vals = jnp.concatenate([biased(pv_ref[...], kb_ref, KVH + j), ov_ref[...]], 0)
    both = jnp.concatenate([keys, vals], 1)
    allow = lax.broadcasted_iota(jnp.int32, (RESP, RESP), 0) <= lax.broadcasted_iota(jnp.int32, (RESP, RESP), 1)
    for h in range(GROUP):
        cols = slice(h * HD, (h + 1) * HD)
        raw = raw_pair(both, q_ref[:, cols], g_ref[:, cols])
        s = raw[:, :RESP]
        dp = raw[:, RESP:]
        s = jnp.concatenate([s[:PRE], jnp.where(allow, s[PRE:], NEG_BIG)], 0)
        e = jnp.exp2((s - jnp.max(s, 0, keepdims=True)) * SCALE)
        p = e * (1.0 / jnp.sum(e, 0, keepdims=True))
        row = jnp.sum(p * dp, 0, keepdims=True)
        pt_ref[:, cols] = p.astype(BF16)
        ds_ref[:, cols] = (p * (dp - row)).astype(BF16)
    pt = pt_ref[...]
    ds = ds_ref[...]
    dk = dot(ds, stacked(q_ref), ((1,), (0,))) * FACTOR
    dv = dot(pt, stacked(g_ref), ((1,), (0,)))
    col = pl.multiple_of(j * HD, HD)
    own_ref[:, pl.ds(col, HD)] = dk[PRE:].astype(BF16)
    own_ref[:, pl.ds(col + WIDTH, HD)] = dv[PRE:].astype(BF16)
    at = pl.multiple_of(j * ROWS, ROWS)
    pre_ref[:, pl.ds(at, ROWS), :] = dk[:PRE].astype(BF16).reshape(PEERS, ROWS, HD)
    pre_ref[:, pl.ds(at + KVH * ROWS, ROWS), :] = dv[:PRE].astype(BF16).reshape(PEERS, ROWS, HD)
    dq = dot(ds, keys, ((0,), (0,))) * FACTOR
    out = dot(pt, vals, ((0,), (0,)))
    live = lax.broadcasted_iota(jnp.int32, (RESP, HD), 0) < len_ref[0, 0]
    for h in range(GROUP):
        cols = slice(h * HD, (h + 1) * HD)
        rows = slice(h * RESP, (h + 1) * RESP)
        att_ref[:, cols] = jnp.where(live, out[rows], 0.0).astype(BF16)
        dq_ref[:, cols] = dq[rows].astype(BF16)


def enclose_kernel(buffer_ref, parts_ref, out_ref):
    del buffer_ref
    total = jnp.sum(parts_ref[...], 0)
    rows = jnp.concatenate([*in_three(total), jnp.zeros((2, HD), F32)], 0).astype(BF16)
    out_ref[...] = jnp.broadcast_to(rows[None], (PEERS, 8, HD))


def finish_kernel(arrived_ref, pre_ref, q_ref, kv_ref):
    for m in range(2 * KVH):
        piece = arrived_ref[:, m * ROWS:(m + 1) * ROWS, :].astype(F32)
        pre_ref[:, m * HD:(m + 1) * HD] = jnp.sum(piece, 0).astype(BF16)
    for i in range((QH + 2 * KVH) // 2):
        tail = arrived_ref[i, CHUNK:, :].astype(F32)
        pair = tail[0:2] + tail[2:4] + tail[4:6]
        if 2 * i < QH:
            q_ref[2 * i:2 * i + 2, :] = pair
        else:
            kv_ref[2 * i - QH:2 * i - QH + 2, :] = pair


def first(j):
    return 0, j


def second(j):
    return 0, KVH + j


def whole(j):
    return 0, 0


def params():
    return pltpu.CompilerParams(dimension_semantics=("arbitrary",), vmem_limit_bytes=VMEM_LIMIT)


def cost(matmuls):
    return pl.CostEstimate(
        flops=matmuls * 2 * QH * RESP * KEYS * HD, bytes_accessed=4_000_000, transcendentals=QH * RESP * KEYS
    )


def own(length, query, out_grad, resp_kv, query_bias, kv_bias):
    wide = pl.BlockSpec((RESP, GW), first)
    return pl.pallas_call(
        own_kernel,
        grid=(KVH,),
        in_specs=[
            pl.BlockSpec(memory_space=pltpu.SMEM),
            wide,
            wide,
            pl.BlockSpec((RESP, HD), first),
            pl.BlockSpec((RESP, HD), second),
            pl.BlockSpec((QH, HD), whole),
            pl.BlockSpec((2 * KVH, HD), whole),
        ],
        out_specs=[
            wide,
            wide,
            pl.BlockSpec((RESP, 2 * WIDTH), lambda j: (0, 0)),
            wide,
            wide,
            pl.BlockSpec((1, 8, GW), lambda j: (j, 0, 0)),
        ],
        out_shape=[
            jax.ShapeDtypeStruct((RESP, QH * HD), BF16),
            jax.ShapeDtypeStruct((RESP, QH * HD), BF16),
            jax.ShapeDtypeStruct((RESP, 2 * WIDTH), BF16),
            pltpu.HBM((RESP, QH * HD), F32),
            pltpu.HBM((RESP, QH * HD), F32),
            jax.ShapeDtypeStruct((KVH, 8, GW), F32),
        ],
        compiler_params=params(),
        cost_estimate=cost(1),
        name="own",
    )(length, query, out_grad, resp_kv, resp_kv, query_bias, kv_bias)


def score(q, g, prefix, kv_bias, own_kv, e, dp, stat):
    wide = pl.BlockSpec((RESP, GW), first)
    return pl.pallas_call(
        score_kernel,
        grid=(KVH,),
        in_specs=[
            wide,
            wide,
            pl.BlockSpec((PRE, HD), first),
            pl.BlockSpec((PRE, HD), second),
            pl.BlockSpec((2 * KVH, HD), whole),
            pl.BlockSpec((RESP, HD), first),
            wide,
            wide,
            pl.BlockSpec((1, 8, GW), lambda j: (j, 0, 0)),
        ],
        out_specs=pl.BlockSpec((32, 2, HD), lambda j: (0, 0, 0)),
        out_shape=jax.ShapeDtypeStruct((32, 2, HD), F32),
        scratch_shapes=[pltpu.VMEM((GROUP, PRE, 2 * RESP), F32), pltpu.VMEM((KEYS, GW), BF16)],
        compiler_params=params(),
        cost_estimate=cost(3),
        name="score",
    )(q, g, prefix, prefix, kv_bias, own_kv, e, dp, stat)


def grads(length, q, g, prefix, kv_bias, own_kv):
    wide = pl.BlockSpec((RESP, GW), first)
    return pl.pallas_call(
        grad_kernel,
        grid=(KVH,),
        in_specs=[
            pl.BlockSpec(memory_space=pltpu.SMEM),
            wide,
            wide,
            pl.BlockSpec((PRE, HD), first),
            pl.BlockSpec((PRE, HD), second),
            pl.BlockSpec((2 * KVH, HD), whole),
            pl.BlockSpec((RESP, HD), first),
            pl.BlockSpec((RESP, HD), second),
        ],
        out_specs=[
            wide,
            wide,
            pl.BlockSpec((RESP, 2 * WIDTH), whole),
            pl.BlockSpec((PEERS, CHUNK + 8, HD), lambda j: (0, 0, 0)),
        ],
        out_shape=[
            jax.ShapeDtypeStruct((RESP, QH * HD), BF16),
            jax.ShapeDtypeStruct((RESP, QH * HD), BF16),
            jax.ShapeDtypeStruct((RESP, 2 * WIDTH), BF16),
            jax.ShapeDtypeStruct((PEERS, CHUNK + 8, HD), BF16),
        ],
        scratch_shapes=[pltpu.VMEM((KEYS, GW), BF16), pltpu.VMEM((KEYS, GW), BF16)],
        compiler_params=params(),
        cost_estimate=cost(6),
        name="grads",
    )(length, q, g, prefix, prefix, kv_bias, own_kv, own_kv)


def enclose(pre, parts):
    return pl.pallas_call(
        enclose_kernel,
        grid=(1,),
        in_specs=[pl.BlockSpec(memory_space=pl.ANY), pl.BlockSpec((32, 2, HD), lambda i: (0, 0, 0))],
        out_specs=pl.BlockSpec((PEERS, 8, HD), lambda i: (0, CHUNK // 8, 0)),
        out_shape=jax.ShapeDtypeStruct(pre.shape, BF16),
        input_output_aliases={0: 0},
        compiler_params=params(),
        name="enclose",
    )(pre, parts)


def finish(arrived):
    return pl.pallas_call(
        finish_kernel,
        out_shape=[
            jax.ShapeDtypeStruct((ROWS, 2 * WIDTH), BF16),
            jax.ShapeDtypeStruct((QH, HD), F32),
            jax.ShapeDtypeStruct((2 * KVH, HD), F32),
        ],
        compiler_params=pltpu.CompilerParams(vmem_limit_bytes=VMEM_LIMIT),
        name="finish",
    )(arrived)


def in_hbm(x):
    return pltpu.with_memory_space_constraint(x, pltpu.HBM)


def exchange(pieces, axes):
    return lax.all_to_all(pieces, axes, 0, 0, tiled=True)


def local(query, resp_kv, prefix_kv, query_bias, kv_bias, out_grad, lengths):
    query_bias = query_bias.reshape(QH, HD)
    kv_bias = kv_bias.reshape(2 * KVH, HD)
    prefix = exchange(jnp.broadcast_to(prefix_kv[0], (PEERS, ROWS, 2 * WIDTH)), GRP).reshape(PRE, 2 * WIDTH)
    q, g, own_kv, e, dp, stat = own(lengths, in_hbm(query[0]), in_hbm(out_grad[0]), in_hbm(resp_kv[0]), query_bias, kv_bias)
    bias = score(q, g, prefix, kv_bias, own_kv, in_hbm(e), in_hbm(dp), stat)
    part = jnp.sum(exchange(bias, PLANE), 0)
    part, lengths = lax.optimization_barrier((part, lengths))
    att, dq, own_grad, pre = grads(lengths, q, g, prefix, kv_bias, own_kv)
    order = [(i + 22) % 32 for i in range(32)]
    part = lax.all_to_all(
        jnp.broadcast_to(part, (32, 2, HD)), COLUMN, 0, 0, axis_index_groups=[order], tiled=True
    )
    pre_grad, qsum, kvsum = finish(exchange(enclose(pre, part), GRP))
    return (
        att[None],
        dq[None],
        own_grad[None],
        pre_grad[None],
        qsum.reshape(QH * HD),
        kvsum.reshape(2 * WIDTH),
    )


def solution(mesh):
    finer = Mesh(mesh.devices.reshape(2, 4, 2, 32, 2), ("grp_0", "grp_1", "grp_2", "dp_0", "dp_1"))
    rows = P(DP, GRP, None)
    return jax.shard_map(
        local,
        mesh=finer,
        in_specs=(rows, rows, rows, P(), P(), rows, P(DP, GRP)),
        out_specs=(rows, rows, rows, rows, P(), P()),
        check_vma=False,
    )
```
